32 devices in a mesh: rows: 8 (over z, y), mem: 4 (over x, core).
Axes of the slice: x: 2, y: 2, z: 4, core: 2. Of those that a mesh axis runs over, the one named last changes fastest.
Arguments:
- ensemble: float32 [64, 32, 48, 384], P('mem', None, 'rows'), may hold values from 0 to 2
- courant: float32 [3, 32, 48, 384], P(None, None, 'rows'), may hold values from -0.22 to 0.22
- obs_column: int32 [128], P('rows'), may hold values from 0 to 18431, as said below
- obs_value: float32 [32, 128], P(None, 'rows'), may hold values from -6 to 6
- obs_var: float32 [32, 128], P(None, 'rows'), may hold values from 0.5 to 8
Outputs:
- analysis: float32 [64, 32, 48, 384], P('mem', None, 'rows')
The draws below stay inside these ranges and needn't reach their ends.
Inputs may be any that keep to these rules, and one draw needn't show every extreme that they name: `obs_column`: entry p is x * 384 + y with x from (p // 16) * 6 to (p // 16) * 6 + 5.
All inputs are finite; a program needn't handle non-finite values.
Results may differ from the reference program's by a relative error of at most 0.0003.
Values sent between devices are 32-bit elements; how exact they have to be, the bound alone decides.
A program may use at most 128 MiB of HBM per device.

```python
import math
import jax
import jax.numpy as jnp
from jax import lax

ENSEMBLE_SIZE = 64
VERTICAL_COUNT = 32
ROW_CELLS = 384
RX = 6
PROF_DEV = 16
STEPS = 3
NS_ITERS = 4
GRID_ROWS = 48
NPROF = 128


def draw_obs_column(key, part):
    first_key, second_key = jax.random.split(jax.random.fold_in(key, 11))
    owner = jnp.arange(NPROF, dtype=jnp.int32) // PROF_DEV
    row_offset = jax.random.randint(first_key, (NPROF,), 0, RX, dtype=jnp.int32)
    column_y = jax.random.randint(second_key, (NPROF,), 0, ROW_CELLS, dtype=jnp.int32)
    return ((owner * RX + row_offset) * ROW_CELLS + column_y).astype(jnp.int32)


def block_levels(rng, extent, pieces, low, largest):
    loudness, own = 1.0, jax.random.fold_in(rng, 6)
    for dim, parts in pieces:
        heights = jnp.exp(jax.random.uniform(jax.random.fold_in(own, dim), (parts,), jnp.float32, low / len(pieces), largest / len(pieces)))
        loudness = loudness * jnp.repeat(heights, extent[dim] // parts).reshape([-1 if axis == dim else 1 for axis in range(len(extent))])
    return loudness


def bell_draw(key, extent, spread, limit, cuts=(), held_as=jnp.bfloat16):
    drawn = spread * jax.random.normal(key, extent, jnp.float32)
    if cuts:
        drawn = drawn * block_levels(key, extent, cuts, -0.22, 0.18)
    return jnp.clip(drawn, -limit, limit).astype(held_as)


def setup_inputs(seed: int = 0) -> dict:
    key_list = jax.random.split(jax.random.key(seed), 6)
    ensemble = jnp.clip(2.0 * jax.random.uniform(key_list[0], (ENSEMBLE_SIZE, VERTICAL_COUNT, GRID_ROWS, ROW_CELLS), jnp.float32) ** block_levels(key_list[0], (ENSEMBLE_SIZE, VERTICAL_COUNT, GRID_ROWS, ROW_CELLS), ((0, 4), (2, 8)), -0.2, 0.2), 0.0, 2.0)
    courant = jnp.clip(jax.random.uniform(key_list[1], (3, VERTICAL_COUNT, GRID_ROWS, ROW_CELLS), jnp.float32, -0.22, 0.22) * block_levels(key_list[1], (3, VERTICAL_COUNT, GRID_ROWS, ROW_CELLS), ((2, 8),), -0.4, 0.0), -0.22, 0.22)
    obs_column = draw_obs_column(jax.random.fold_in(key_list[5], 71), 0)
    obs_value = bell_draw(key_list[3], (VERTICAL_COUNT, NPROF), 1.0, 6.0, ((1, 8),), jnp.float32)
    obs_var = jnp.clip(jnp.exp(math.log(8.0) - 2.7725887 * jax.random.uniform(key_list[4], (VERTICAL_COUNT, NPROF), jnp.float32) ** block_levels(key_list[4], (VERTICAL_COUNT, NPROF), ((1, 8),), -0.2, 0.2)), 0.5, 8.0)
    return {"ensemble": ensemble, "courant": courant, "obs_column": obs_column, "obs_value": obs_value, "obs_var": obs_var}


DIFFUSION = 0.05

def advance(padded, courant):
    center = padded[:, :, 1:-1, :]
    below_x = padded[:, :, :-2, :]
    above_x = padded[:, :, 2:, :]
    padded_y = jnp.pad(center, ((0, 0), (0, 0), (0, 0), (1, 1)))
    below_y = padded_y[:, :, :, :-2]
    above_y = padded_y[:, :, :, 2:]
    padded_z = jnp.pad(center, ((0, 0), (1, 1), (0, 0), (0, 0)))
    below_z = padded_z[:, :-2]
    above_z = padded_z[:, 2:]
    change = jnp.zeros_like(center)
    for component, below, above in ((0, below_x, above_x), (1, below_y, above_y), (2, below_z, above_z)):
        velocity = courant[component][None]
        change = change - jnp.maximum(velocity, 0.0) * (center - below) - jnp.minimum(velocity, 0.0) * (above - center) + DIFFUSION * (above + below - 2.0 * center)
    return center + change

def gram_terms(profiles, obs_value, obs_var):
    members_all = profiles.shape[0]
    center = lax.optimization_barrier(jnp.mean(profiles, axis=0))
    scaling = 1.0 / jnp.sqrt((members_all - 1.0) * obs_var)
    scaled = ((profiles - center[None]) * scaling[None]).reshape(members_all, -1)
    innovation = ((obs_value - center) / jnp.sqrt(obs_var)).reshape(-1)
    gram_part = jnp.dot(scaled, scaled.T, precision=lax.Precision.HIGHEST)
    pull_part = jnp.dot(scaled, innovation, precision=lax.Precision.HIGHEST)
    return (gram_part, pull_part)

def mixing(gram_sum, pull_sum):
    members_all = gram_sum.shape[0]
    identity_matrix = jnp.eye(members_all, dtype=jnp.float32)
    system = identity_matrix + gram_sum
    frobenius = jnp.sqrt(jnp.sum(system * system))

    def newton(iteration, carry):
        iterate, inverse_root = carry
        factor = 0.5 * (3.0 * identity_matrix - jnp.dot(inverse_root, iterate, precision=lax.Precision.HIGHEST))
        return (jnp.dot(iterate, factor, precision=lax.Precision.HIGHEST), jnp.dot(factor, inverse_root, precision=lax.Precision.HIGHEST))
    iterate, inverse_root = lax.fori_loop(0, NS_ITERS, newton, (system / frobenius, identity_matrix))
    root_inverse = inverse_root / jnp.sqrt(frobenius)
    mean_shift = jnp.dot(root_inverse, jnp.dot(root_inverse, pull_sum, precision=lax.Precision.HIGHEST), precision=lax.Precision.HIGHEST) / jnp.sqrt(members_all - 1.0)
    centering = identity_matrix - 1.0 / members_all
    return 1.0 / members_all + jnp.dot(centering, mean_shift[:, None] + root_inverse, precision=lax.Precision.HIGHEST)

def reference(ensemble, courant, obs_column, obs_value, obs_var):

    def prior_state(member_index):
        concentration = member_index[None]
        for counter in range(STEPS):
            padded = jnp.pad(concentration, ((0, 0), (0, 0), (1, 1), (0, 0)))
            concentration = advance(padded, courant)
        return concentration[0]
    prior_states = lax.map(prior_state, ensemble)
    state_vectors = prior_states.reshape(ENSEMBLE_SIZE, VERTICAL_COUNT, GRID_ROWS * ROW_CELLS)
    profiles = jnp.take(state_vectors, obs_column, axis=2)
    gram_sum, pull_sum = gram_terms(profiles, obs_value, obs_var)
    transform_weights = mixing(gram_sum, pull_sum)
    updated_ensemble = jnp.dot(transform_weights.T, prior_states.reshape(ENSEMBLE_SIZE, -1), precision=lax.Precision.HIGHEST)
    return updated_ensemble.reshape(ensemble.shape)
```

```python
import functools

import jax
import jax.numpy as jnp
from jax import lax
from jax.experimental import pallas as pl
from jax.experimental.pallas import tpu as pltpu
from jax.sharding import PartitionSpec as P

STEPS = 3
NS_ITERS = 4
DIFFUSION = 0.05
LANES = 128
MESH = pl.DeviceIdType.MESH
HIGHEST = lax.Precision.HIGHEST


def kernel(
    rows_n, mem_n,
    ens, cour, obs_x, obs_y, obs_value, obs_var,
    out,
    chalo, hal, coef, w0, w1, w2, w3, fc, st, prof, grec, wts, wts_s,
    c_send, c_recv, cf_send, cf_recv, h_send, h_recv,
    x_send, p_send, f_recv, q_send, q_recv, g_send, g_recv, w_sem,
):
    members, rows, levels, width = ens.shape
    total = members * mem_n
    nobs = obs_x.shape[0]
    chips = mem_n // 2
    row = lax.axis_index("rows")
    mem = lax.axis_index("mem")
    core = lax.rem(mem, 2)
    chip = mem // 2
    partner = chip * 2 + 1 - core

    def dev(r, m):
        return {"rows": r, "mem": m}

    def remote(src, dst, ssem, rsem, r, m):
        return pltpu.make_async_remote_copy(
            src_ref=src, dst_ref=dst, send_sem=ssem, recv_sem=rsem,
            device_id=(r, m), device_id_type=MESH,
        )

    barrier = pltpu.get_barrier_semaphore()
    for d in range(1, mem_n):
        pl.semaphore_signal(barrier, inc=1, device_id=(row, lax.rem(mem + d, mem_n)), device_id_type=MESH)
    for d in range(1, rows_n):
        pl.semaphore_signal(barrier, inc=1, device_id=(lax.rem(row + d, rows_n), mem), device_id_type=MESH)
    pl.semaphore_wait(barrier, mem_n - 1 + rows_n - 1)

    has_low = row > 0
    has_high = row < rows_n - 1
    low = jnp.maximum(row - 1, 0)
    high = jnp.minimum(row + 1, rows_n - 1)

    def chalo_up():
        return remote(cour.at[rows - 2 + core], chalo.at[0, core], c_send.at[0], c_recv.at[0], high, mem)

    def chalo_down():
        return remote(cour.at[core], chalo.at[1, core], c_send.at[1], c_recv.at[1], low, mem)

    def chalo_pass(side):
        return remote(chalo.at[side, core], chalo.at[side, core], cf_send.at[side], cf_recv.at[side], row, partner)

    def halo_up(m):
        return remote(ens.at[m, pl.ds(rows - 3, 3)], hal.at[m, 0], h_send.at[0, m], h_recv.at[0, m], high, mem)

    def halo_down(m):
        return remote(ens.at[m, pl.ds(0, 3)], hal.at[m, 1], h_send.at[1, m], h_recv.at[1, m], low, mem)

    @pl.when(has_high)
    def _():
        chalo_up().start()

    @pl.when(has_low)
    def _():
        chalo_down().start()

    @pl.loop(0, members)
    def _(m):
        @pl.when(has_high)
        def _():
            halo_up(m).start()

        @pl.when(has_low)
        def _():
            halo_down(m).start()

    level = lax.broadcasted_iota(jnp.int32, (levels, width), 0)
    cell = lax.broadcasted_iota(jnp.int32, (levels, width), 1)

    def set_coef(i, a0, a1, a2):
        coef[i, 0] = 1.0 - 6.0 * DIFFUSION - jnp.abs(a0) - jnp.abs(a1) - jnp.abs(a2)
        coef[i, 1] = DIFFUSION + jnp.maximum(a0, 0.0)
        coef[i, 2] = DIFFUSION - jnp.minimum(a0, 0.0)
        coef[i, 3] = jnp.where(cell > 0, DIFFUSION + jnp.maximum(a1, 0.0), 0.0)
        coef[i, 4] = jnp.where(cell < width - 1, DIFFUSION - jnp.minimum(a1, 0.0), 0.0)
        coef[i, 5] = jnp.where(level > 0, DIFFUSION + jnp.maximum(a2, 0.0), 0.0)
        coef[i, 6] = jnp.where(level < levels - 1, DIFFUSION - jnp.minimum(a2, 0.0), 0.0)

    @pl.loop(0, rows)
    def _(i):
        set_coef(i + 2, cour[i, 0], cour[i, 1], cour[i, 2])

    st[...] = jnp.zeros_like(st)

    def edge(side, present, first):
        @pl.when(present)
        def _():
            (chalo_down if side else chalo_up)().wait_recv()
            chalo_pass(side).start()
            chalo_pass(side).wait_recv()

            @pl.loop(0, 2)
            def _(i):
                set_coef(first + i, chalo[side, i, 0], chalo[side, i, 1], chalo[side, i, 2])

        @pl.when(jnp.logical_not(present))
        def _():
            coef[pl.ds(first, 2)] = jnp.zeros((2, 7, levels, width), jnp.float32)

    edge(0, has_low, 0)
    edge(1, has_high, rows + 2)

    @pl.when(jnp.logical_not(has_low))
    def _():
        w0[pl.ds(0, 3)] = jnp.zeros((3, levels, width), jnp.float32)

    @pl.when(jnp.logical_not(has_high))
    def _():
        w0[pl.ds(rows + 3, 3)] = jnp.zeros((3, levels, width), jnp.float32)

    def update(src, i, c):
        mid = src[i + 1]
        return (
            coef[c, 0] * mid
            + coef[c, 1] * src[i]
            + coef[c, 2] * src[i + 2]
            + coef[c, 3] * pltpu.roll(mid, 1, 1)
            + coef[c, 4] * pltpu.roll(mid, width - 1, 1)
            + coef[c, 5] * pltpu.roll(mid, 1, 0)
            + coef[c, 6] * pltpu.roll(mid, levels - 1, 0)
        )

    def other(d):
        return lax.rem(chip + d, chips) * 2 + core

    def send_x(d, m):
        slot = fc.at[mem * members + m]
        return remote(slot, slot, x_send.at[d, m], f_recv.at[mem, m], row, other(d))

    def send_p(d, m):
        src = lax.rem(chip + d, chips) * 2 + core
        slot = fc.at[src * members + m]
        return remote(slot, slot, p_send.at[d, m], f_recv.at[src, m], row, partner)

    def arrived(src, m):
        slot = fc.at[src * members + m]
        return remote(slot, slot, p_send.at[0, 0], f_recv.at[src, m], row, partner)

    def forward(m):
        for d in range(1, chips):
            arrived(other(d), m).wait_recv()
            send_p(d, m).start()

    lane = lax.broadcasted_iota(jnp.int32, (levels, LANES), 1)
    lag = 2

    @pl.loop(0, members)
    def _(m):
        @pl.when(has_low)
        def _():
            halo_up(m).wait_recv()
            w0[pl.ds(0, 3)] = hal[m, 0]

        @pl.when(has_high)
        def _():
            halo_down(m).wait_recv()
            w0[pl.ds(rows + 3, 3)] = hal[m, 1]

        w0[pl.ds(3, rows)] = ens[m]

        @pl.loop(0, rows + 4)
        def _(i):
            w1[i] = update(w0, i, i)

        @pl.loop(0, rows + 2)
        def _(i):
            w2[i] = update(w1, i, i + 1)

        @pl.loop(0, rows)
        def _(i):
            value = update(w2, i, i + 2)
            w3[i] = value
            fc[mem * members + m, i] = value

        @pl.loop(0, nobs)
        def _(p):
            plane = w3[obs_x[p]]
            picked = jnp.sum(jnp.where(cell == obs_y[p], plane, 0.0), axis=1, keepdims=True)
            where = pl.ds(pl.multiple_of(p * levels, levels), levels)
            st[where] = jnp.where(lane == m, picked, st[where])

        for d in range(1, chips):
            send_x(d, m).start()
        send_p(0, m).start()

        @pl.when(m >= lag)
        def _():
            forward(m - lag)

    mine = pl.ds(pl.multiple_of(mem * members, members), members)
    prof[mine] = st[...].T[:members]
    for d in range(1, mem_n):
        remote(prof.at[mine], prof.at[mine], q_send.at[d], q_recv.at[mem], row, lax.rem(mem + d, mem_n)).start()
    for d in range(1, mem_n):
        src = lax.rem(mem + d, mem_n)
        block = prof.at[pl.ds(pl.multiple_of(src * members, members), members)]
        remote(block, block, q_send.at[d], q_recv.at[src], row, src).wait_recv()

    values = prof[...]
    center = jnp.mean(values, axis=0, keepdims=True)
    scaled = (values - center) / jnp.sqrt((total - 1.0) * obs_var[...])
    innovation = (obs_value[...] - center) / jnp.sqrt(obs_var[...])
    pad = jnp.broadcast_to(innovation, (LANES - total, innovation.shape[1]))
    both = jnp.concatenate([scaled, pad], axis=0)
    grec[row] = lax.dot_general(
        scaled, both, (((1,), (1,)), ((), ())), precision=HIGHEST, preferred_element_type=jnp.float32
    )
    for d in range(1, rows_n):
        remote(grec.at[row], grec.at[row], g_send.at[d], g_recv.at[row], lax.rem(row + d, rows_n), mem).start()

    forward(members - 2)
    forward(members - 1)

    for d in range(1, rows_n):
        src = lax.rem(row + d, rows_n)
        remote(grec.at[src], grec.at[src], g_send.at[d], g_recv.at[src], src, mem).wait_recv()
    gsum = grec[0]
    for r in range(1, rows_n):
        gsum = gsum + grec[r]

    def dot(a, b):
        return jnp.dot(a, b, precision=HIGHEST, preferred_element_type=jnp.float32)

    ri = lax.broadcasted_iota(jnp.int32, (total, total), 0)
    ci = lax.broadcasted_iota(jnp.int32, (total, total), 1)
    eye = jnp.where(ri == ci, 1.0, 0.0).astype(jnp.float32)
    system = eye + gsum[:, :total]
    frob = jnp.sqrt(jnp.sum(jnp.sum(system * system, axis=1, keepdims=True), axis=0, keepdims=True))
    y = system / frob
    z = eye
    for it in range(NS_ITERS):
        factor = 0.5 * (3.0 * eye - (y if it == 0 else dot(z, y)))
        if it < NS_ITERS - 1:
            y = dot(y, factor)
        z = factor if it == 0 else dot(factor, z)
    root = z / jnp.sqrt(frob)
    shift = dot(root, dot(root, gsum))[:, total:total + 1] / jnp.sqrt(jnp.float32(total - 1.0))
    mixed = shift + root
    weights = 1.0 / total + mixed - jnp.mean(mixed, axis=0, keepdims=True)
    wts[...] = weights.T
    fetch = pltpu.make_async_copy(wts.at[mine], wts_s, w_sem)
    fetch.start()
    fetch.wait()

    for d in range(chips):
        src = lax.rem(chip + d, chips) * 2 + 1 - core

        @pl.loop(0, members)
        def _(m):
            arrived(src, m).wait_recv()

    per = 8

    @pl.loop(0, rows * (levels // per))
    def _(n):
        i = n // (levels // per)
        where = pl.ds(pl.multiple_of(lax.rem(n, levels // per) * per, per), per)

        for first in range(0, members, 16):
            count = min(16, members - first)

            def add(j, acc):
                f = fc[j, i, where]
                return tuple(acc[k] + wts_s[first + k, j] * f for k in range(count))

            acc = lax.fori_loop(
                0, total, add, tuple(jnp.zeros((per, width), jnp.float32) for _ in range(count)), unroll=2
            )
            for k in range(count):
                out[first + k, i, where] = acc[k]

    @pl.when(has_high)
    def _():
        chalo_up().wait_send()
        chalo_pass(1).wait_send()

    @pl.when(has_low)
    def _():
        chalo_down().wait_send()
        chalo_pass(0).wait_send()

    @pl.loop(0, members)
    def _(m):
        @pl.when(has_high)
        def _():
            halo_up(m).wait_send()

        @pl.when(has_low)
        def _():
            halo_down(m).wait_send()

        for d in range(1, chips):
            send_x(d, m).wait_send()
        for d in range(chips):
            send_p(d, m).wait_send()

    for d in range(1, mem_n):
        remote(prof.at[mine], prof.at[mine], q_send.at[d], q_recv.at[mem], row, lax.rem(mem + d, mem_n)).wait_send()
    for d in range(1, rows_n):
        remote(grec.at[row], grec.at[row], g_send.at[d], g_recv.at[row], lax.rem(row + d, rows_n), mem).wait_send()


def per_device(rows_n, mem_n, ensemble, courant, obs_column, obs_value, obs_var):
    members, levels, rows, width = ensemble.shape
    nobs = obs_column.shape[0]
    chips = mem_n // 2
    local = obs_column - lax.axis_index("rows") * (rows * width)
    f32 = jnp.float32
    vmem = pl.BlockSpec(memory_space=pltpu.VMEM)
    smem = pl.BlockSpec(memory_space=pltpu.SMEM)
    dma = pltpu.SemaphoreType.DMA
    total = members * mem_n
    plane = (levels, width)
    result = pl.pallas_call(
        functools.partial(kernel, rows_n, mem_n),
        out_shape=jax.ShapeDtypeStruct((members, rows, levels, width), f32),
        in_specs=[vmem, vmem, smem, smem, vmem, vmem],
        out_specs=vmem,
        scratch_shapes=[
            pltpu.VMEM((2, 2, 3) + plane, f32),
            pltpu.VMEM((members, 2, 3) + plane, f32),
            pltpu.VMEM((rows + 4, 7) + plane, f32),
            pltpu.VMEM((rows + 6,) + plane, f32),
            pltpu.VMEM((rows + 4,) + plane, f32),
            pltpu.VMEM((rows + 2,) + plane, f32),
            pltpu.VMEM((rows,) + plane, f32),
            pltpu.VMEM((total, rows) + plane, f32),
            pltpu.VMEM((nobs * levels, LANES), f32),
            pltpu.VMEM((total, nobs * levels), f32),
            pltpu.VMEM((rows_n, total, LANES), f32),
            pltpu.VMEM((total, total), f32),
            pltpu.SMEM((members, total), f32),
            dma((2,)), dma((2,)), dma((2,)), dma((2,)),
            dma((2, members)), dma((2, members)),
            dma((chips, members)), dma((chips, members)), dma((mem_n, members)),
            dma((mem_n,)), dma((mem_n,)),
            dma((rows_n,)), dma((rows_n,)),
            dma,
        ],
        compiler_params=pltpu.CompilerParams(
            collective_id=0, has_side_effects=True, vmem_limit_bytes=60 * 1024 * 1024
        ),
    )(
        ensemble.transpose(0, 2, 1, 3),
        courant.transpose(2, 0, 1, 3),
        local // width,
        local % width,
        obs_value.T.reshape(1, -1),
        obs_var.T.reshape(1, -1),
    )
    return result.transpose(0, 2, 1, 3)


def solution(mesh):
    return jax.shard_map(
        functools.partial(per_device, mesh.shape["rows"], mesh.shape["mem"]),
        mesh=mesh,
        in_specs=(
            P("mem", None, "rows", None),
            P(None, None, "rows", None),
            P("rows"),
            P(None, "rows"),
            P(None, "rows"),
        ),
        out_specs=P("mem", None, "rows", None),
        check_vma=False,
    )
```

```python
import functools

import jax
import jax.numpy as jnp
from jax import lax
from jax.experimental import pallas as pl
from jax.experimental.pallas import tpu as pltpu
from jax.sharding import PartitionSpec as P

STEPS = 3
NS_ITERS = 4
DIFFUSION = 0.05
AHEAD = 2
LANES = 128
MESH = pl.DeviceIdType.MESH
HIGHEST = lax.Precision.HIGHEST


def kernel(
    rows_n, mem_n,
    ens, cour, obs_x, obs_y, obs_value, obs_var,
    out,
    chalo, hal, coef, w0, w1, w2, w3, fc, st, prof, grec, wts,
    c_send, c_recv, cf_send, cf_recv, h_send, h_recv,
    x_send, p_send, f_recv, q_send, q_recv, g_send, g_recv,
):
    members, rows, levels, width = ens.shape
    total = members * mem_n
    nobs = obs_x.shape[0]
    chips = mem_n // 2
    row = lax.axis_index("rows")
    mem = lax.axis_index("mem")
    core = lax.rem(mem, 2)
    chip = mem // 2
    partner = chip * 2 + 1 - core

    def dev(r, m):
        return {"rows": r, "mem": m}

    def remote(src, dst, ssem, rsem, r, m):
        return pltpu.make_async_remote_copy(
            src_ref=src, dst_ref=dst, send_sem=ssem, recv_sem=rsem,
            device_id=(r, m), device_id_type=MESH,
        )

    barrier = pltpu.get_barrier_semaphore()
    for d in range(1, mem_n):
        pl.semaphore_signal(barrier, inc=1, device_id=(row, lax.rem(mem + d, mem_n)), device_id_type=MESH)
    for d in range(1, rows_n):
        pl.semaphore_signal(barrier, inc=1, device_id=(lax.rem(row + d, rows_n), mem), device_id_type=MESH)
    pl.semaphore_wait(barrier, mem_n - 1 + rows_n - 1)

    has_low = row > 0
    has_high = row < rows_n - 1
    low = jnp.maximum(row - 1, 0)
    high = jnp.minimum(row + 1, rows_n - 1)

    def chalo_up():
        return remote(cour.at[:, rows - 2 + core], chalo.at[0, core], c_send.at[0], c_recv.at[0], high, mem)

    def chalo_down():
        return remote(cour.at[:, core], chalo.at[1, core], c_send.at[1], c_recv.at[1], low, mem)

    def chalo_pass(side):
        return remote(chalo.at[side, core], chalo.at[side, core], cf_send.at[side], cf_recv.at[side], row, partner)

    def halo_up(m):
        return remote(ens.at[m, pl.ds(rows - 3, 3)], hal.at[m, 0], h_send.at[0, m], h_recv.at[0, m], high, mem)

    def halo_down(m):
        return remote(ens.at[m, pl.ds(0, 3)], hal.at[m, 1], h_send.at[1, m], h_recv.at[1, m], low, mem)

    @pl.when(has_high)
    def _():
        chalo_up().start()

    @pl.when(has_low)
    def _():
        chalo_down().start()

    def send_halo(m):
        @pl.when(has_high)
        def _():
            halo_up(m).start()

        @pl.when(has_low)
        def _():
            halo_down(m).start()

    ahead = min(AHEAD, members)

    @pl.loop(0, ahead)
    def _(m):
        send_halo(m)

    level = lax.broadcasted_iota(jnp.int32, (levels, width), 0)
    cell = lax.broadcasted_iota(jnp.int32, (levels, width), 1)

    def set_coef(i, a0, a1, a2):
        coef[i, 0] = 1.0 - 6.0 * DIFFUSION - jnp.abs(a0) - jnp.abs(a1) - jnp.abs(a2)
        coef[i, 1] = DIFFUSION + jnp.maximum(a0, 0.0)
        coef[i, 2] = DIFFUSION - jnp.minimum(a0, 0.0)
        coef[i, 3] = jnp.where(cell > 0, DIFFUSION + jnp.maximum(a1, 0.0), 0.0)
        coef[i, 4] = jnp.where(cell < width - 1, DIFFUSION - jnp.minimum(a1, 0.0), 0.0)
        coef[i, 5] = jnp.where(level > 0, DIFFUSION + jnp.maximum(a2, 0.0), 0.0)
        coef[i, 6] = jnp.where(level < levels - 1, DIFFUSION - jnp.minimum(a2, 0.0), 0.0)

    @pl.loop(0, rows)
    def _(i):
        set_coef(i + 2, cour[0, i], cour[1, i], cour[2, i])

    st[...] = jnp.zeros_like(st)

    def edge(side, present, first):
        @pl.when(present)
        def _():
            (chalo_down if side else chalo_up)().wait_recv()
            chalo_pass(side).start()
            chalo_pass(side).wait_recv()

            @pl.loop(0, 2)
            def _(i):
                set_coef(first + i, chalo[side, i, 0], chalo[side, i, 1], chalo[side, i, 2])

        @pl.when(jnp.logical_not(present))
        def _():
            coef[pl.ds(first, 2)] = jnp.zeros((2, 7, levels, width), jnp.float32)

    edge(0, has_low, 0)
    edge(1, has_high, rows + 2)

    @pl.when(jnp.logical_not(has_low))
    def _():
        w0[pl.ds(0, 3)] = jnp.zeros((3, levels, width), jnp.float32)

    @pl.when(jnp.logical_not(has_high))
    def _():
        w0[pl.ds(rows + 3, 3)] = jnp.zeros((3, levels, width), jnp.float32)

    def update(src, i, c):
        mid = src[i + 1]
        return (
            coef[c, 0] * mid
            + coef[c, 1] * src[i]
            + coef[c, 2] * src[i + 2]
            + coef[c, 3] * pltpu.roll(mid, 1, 1)
            + coef[c, 4] * pltpu.roll(mid, width - 1, 1)
            + coef[c, 5] * pltpu.roll(mid, 1, 0)
            + coef[c, 6] * pltpu.roll(mid, levels - 1, 0)
        )

    def other(d):
        return lax.rem(chip + d, chips) * 2 + core

    def send_x(d, m):
        slot = fc.at[mem * members + m]
        return remote(slot, slot, x_send.at[d, m], f_recv.at[mem, m], row, other(d))

    def send_p(d, m):
        src = lax.rem(chip + d, chips) * 2 + core
        slot = fc.at[src * members + m]
        return remote(slot, slot, p_send.at[d, m], f_recv.at[src, m], row, partner)

    def arrived(src, m):
        slot = fc.at[src * members + m]
        return remote(slot, slot, p_send.at[0, 0], f_recv.at[src, m], row, partner)

    def forward(m):
        for d in range(1, chips):
            arrived(other(d), m).wait_recv()
            send_p(d, m).start()

    lane = lax.broadcasted_iota(jnp.int32, (levels, LANES), 1)
    lag = 2

    @pl.loop(0, members)
    def _(m):
        @pl.when(has_low)
        def _():
            halo_up(m).wait_recv()
            w0[pl.ds(0, 3)] = hal[m, 0]

        @pl.when(has_high)
        def _():
            halo_down(m).wait_recv()
            w0[pl.ds(rows + 3, 3)] = hal[m, 1]

        @pl.when(m + ahead < members)
        def _():
            send_halo(m + ahead)

        w0[pl.ds(3, rows)] = ens[m]

        @pl.loop(0, rows + 4)
        def _(i):
            w1[i] = update(w0, i, i)

        @pl.loop(0, rows + 2)
        def _(i):
            w2[i] = update(w1, i, i + 1)

        @pl.loop(0, rows)
        def _(i):
            value = update(w2, i, i + 2)
            w3[i] = value
            fc[mem * members + m, i] = value

        @pl.loop(0, nobs)
        def _(p):
            plane = w3[obs_x[p]]
            hit = cell == obs_y[p]
            picked = jnp.sum(jnp.where(hit, plane, 0.0), axis=1, keepdims=True)
            where = pl.ds(pl.multiple_of(p * levels, levels), levels)
            st[where] = jnp.where(lane == m, picked, st[where])

        for d in range(1, chips):
            send_x(d, m).start()
        send_p(0, m).start()

        @pl.when(m >= lag)
        def _():
            forward(m - lag)

    def dot(a, b):
        return jnp.dot(a, b, precision=HIGHEST, preferred_element_type=jnp.float32)

    def flat(ref):
        n = nobs * levels
        spread = lax.broadcasted_iota(jnp.int32, (levels, n), 1) % levels
        spread = jnp.where(spread == lax.broadcasted_iota(jnp.int32, (levels, n), 0), 1.0, 0.0)
        wide = dot(ref[...], spread.astype(jnp.float32))
        owner = lax.broadcasted_iota(jnp.int32, (nobs, n), 1) // levels
        own = owner == lax.broadcasted_iota(jnp.int32, (nobs, n), 0)
        return jnp.sum(jnp.where(own, wide, 0.0), axis=0, keepdims=True)

    mine = pl.ds(pl.multiple_of(mem * members, members), members)
    prof[mine] = st[...].T[:members]
    for d in range(1, mem_n):
        remote(prof.at[mine], prof.at[mine], q_send.at[d], q_recv.at[mem], row, lax.rem(mem + d, mem_n)).start()
    for d in range(1, mem_n):
        src = lax.rem(mem + d, mem_n)
        block = prof.at[pl.ds(pl.multiple_of(src * members, members), members)]
        remote(block, block, q_send.at[d], q_recv.at[src], row, src).wait_recv()

    values = prof[...]
    variance = flat(obs_var)
    center = jnp.mean(values, axis=0, keepdims=True)
    scaled = (values - center) / jnp.sqrt((total - 1.0) * variance)
    innovation = (flat(obs_value) - center) / jnp.sqrt(variance)
    pad = jnp.broadcast_to(innovation, (LANES - total, innovation.shape[1]))
    both = jnp.concatenate([scaled, pad], axis=0)
    grec[row] = lax.dot_general(
        scaled, both, (((1,), (1,)), ((), ())), precision=HIGHEST, preferred_element_type=jnp.float32
    )
    for d in range(1, rows_n):
        remote(grec.at[row], grec.at[row], g_send.at[d], g_recv.at[row], lax.rem(row + d, rows_n), mem).start()

    forward(members - 2)
    forward(members - 1)

    for d in range(1, rows_n):
        src = lax.rem(row + d, rows_n)
        remote(grec.at[src], grec.at[src], g_send.at[d], g_recv.at[src], src, mem).wait_recv()
    gsum = grec[0]
    for r in range(1, rows_n):
        gsum = gsum + grec[r]

    ri = lax.broadcasted_iota(jnp.int32, (total, total), 0)
    ci = lax.broadcasted_iota(jnp.int32, (total, total), 1)
    eye = jnp.where(ri == ci, 1.0, 0.0).astype(jnp.float32)
    system = eye + gsum[:, :total]
    frob = jnp.sqrt(jnp.sum(jnp.sum(system * system, axis=1, keepdims=True), axis=0, keepdims=True))
    y = system / frob
    z = eye
    for it in range(NS_ITERS):
        factor = 0.5 * (3.0 * eye - (y if it == 0 else dot(z, y)))
        if it < NS_ITERS - 1:
            y = dot(y, factor)
        z = factor if it == 0 else dot(factor, z)
    root = z / jnp.sqrt(frob)
    shift = dot(root, dot(root, gsum))[:, total:total + 1] / jnp.sqrt(jnp.float32(total - 1.0))
    mixed = shift + root
    weights = 1.0 / total + mixed - jnp.mean(mixed, axis=0, keepdims=True)
    wts[...] = weights.T
    tile = 8
    outs, ins = members * tile, total * tile

    def hot(shape, dim, size):
        big = lax.broadcasted_iota(jnp.int32, shape, dim) // size
        return jnp.where(big == lax.broadcasted_iota(jnp.int32, shape, 1 - dim), 1.0, 0.0).astype(jnp.float32)

    wide = dot(dot(hot((outs, members), 0, tile), wts[mine]), hot((total, ins), 1, tile))
    same = (
        lax.broadcasted_iota(jnp.int32, (outs, ins), 0) % tile
        == lax.broadcasted_iota(jnp.int32, (outs, ins), 1) % tile
    )
    wide = jnp.where(same, wide, 0.0)
    wide_high = wide.astype(jnp.bfloat16)
    wide_low = (wide - wide_high.astype(jnp.float32)).astype(jnp.bfloat16)

    for d in range(chips):
        src = lax.rem(chip + d, chips) * 2 + 1 - core

        @pl.loop(0, members)
        def _(m):
            arrived(src, m).wait_recv()

    def dot16(a, b):
        return jnp.dot(a, b, preferred_element_type=jnp.float32)

    @pl.loop(0, rows * (levels // tile))
    def _(n):
        i = n // (levels // tile)
        where = pl.ds(pl.multiple_of(lax.rem(n, levels // tile) * tile, tile), tile)
        f = fc[:, i, where].reshape(ins, width)
        f_high = f.astype(jnp.bfloat16)
        f_low = (f - f_high.astype(jnp.float32)).astype(jnp.bfloat16)
        value = dot16(wide_high, f_high) + (dot16(wide_high, f_low) + dot16(wide_low, f_high))
        out[:, i, where] = value.reshape(members, tile, width)

    @pl.when(has_high)
    def _():
        chalo_up().wait_send()
        chalo_pass(1).wait_send()

    @pl.when(has_low)
    def _():
        chalo_down().wait_send()
        chalo_pass(0).wait_send()

    @pl.loop(0, members)
    def _(m):
        @pl.when(has_high)
        def _():
            halo_up(m).wait_send()

        @pl.when(has_low)
        def _():
            halo_down(m).wait_send()

        for d in range(1, chips):
            send_x(d, m).wait_send()
        for d in range(chips):
            send_p(d, m).wait_send()

    for d in range(1, mem_n):
        remote(prof.at[mine], prof.at[mine], q_send.at[d], q_recv.at[mem], row, lax.rem(mem + d, mem_n)).wait_send()
    for d in range(1, rows_n):
        remote(grec.at[row], grec.at[row], g_send.at[d], g_recv.at[row], lax.rem(row + d, rows_n), mem).wait_send()


def per_device(rows_n, mem_n, ensemble, courant, obs_column, obs_value, obs_var):
    members, levels, rows, width = ensemble.shape
    nobs = obs_column.shape[0]
    chips = mem_n // 2
    local = obs_column - lax.axis_index("rows") * (rows * width)
    f32 = jnp.float32
    vmem = pl.BlockSpec(memory_space=pltpu.VMEM)
    smem = pl.BlockSpec(memory_space=pltpu.SMEM)
    dma = pltpu.SemaphoreType.DMA
    total = members * mem_n
    plane = (levels, width)
    result = pl.pallas_call(
        functools.partial(kernel, rows_n, mem_n),
        out_shape=jax.ShapeDtypeStruct((members, rows, levels, width), f32),
        in_specs=[vmem, vmem, smem, smem, vmem, vmem],
        out_specs=vmem,
        scratch_shapes=[
            pltpu.VMEM((2, 2, 3) + plane, f32),
            pltpu.VMEM((members, 2, 3) + plane, f32),
            pltpu.VMEM((rows + 4, 7) + plane, f32),
            pltpu.VMEM((rows + 6,) + plane, f32),
            pltpu.VMEM((rows + 4,) + plane, f32),
            pltpu.VMEM((rows + 2,) + plane, f32),
            pltpu.VMEM((rows,) + plane, f32),
            pltpu.VMEM((total, rows) + plane, f32),
            pltpu.VMEM((nobs * levels, LANES), f32),
            pltpu.VMEM((total, nobs * levels), f32),
            pltpu.VMEM((rows_n, total, LANES), f32),
            pltpu.VMEM((total, total), f32),
            dma((2,)), dma((2,)), dma((2,)), dma((2,)),
            dma((2, members)), dma((2, members)),
            dma((chips, members)), dma((chips, members)), dma((mem_n, members)),
            dma((mem_n,)), dma((mem_n,)),
            dma((rows_n,)), dma((rows_n,)),
        ],
        compiler_params=pltpu.CompilerParams(
            collective_id=0, has_side_effects=True, vmem_limit_bytes=60 * 1024 * 1024
        ),
    )(
        ensemble.transpose(0, 2, 1, 3),
        courant.transpose(0, 2, 1, 3),
        local // width,
        local % width,
        obs_value.T,
        obs_var.T,
    )
    return result.transpose(0, 2, 1, 3)


def solution(mesh):
    return jax.shard_map(
        functools.partial(per_device, mesh.shape["rows"], mesh.shape["mem"]),
        mesh=mesh,
        in_specs=(
            P("mem", None, "rows", None),
            P(None, None, "rows", None),
            P("rows"),
            P(None, "rows"),
            P(None, "rows"),
        ),
        out_specs=P("mem", None, "rows", None),
        check_vma=False,
    )
```

```python
import functools

import jax
import jax.numpy as jnp
from jax import lax
from jax.experimental import pallas as pl
from jax.experimental.pallas import tpu as pltpu
from jax.sharding import PartitionSpec as P

STEPS = 3
NS_ITERS = 4
DIFFUSION = 0.05
AHEAD = 2
LANES = 128
MESH = pl.DeviceIdType.MESH
HIGHEST = lax.Precision.HIGHEST


def kernel(
    rows_n, mem_n,
    ens, cour, obs_x, obs_y, obs_value, obs_var,
    out,
    chalo, hal, coef, w0, w1, w2, w3, fc, st, prof, grec, wts,
    c_send, c_recv, cf_send, cf_recv, h_send, h_recv,
    x_send, p_send, f_recv, q_send, q_recv, g_send, g_recv,
):
    members, rows, levels, width = ens.shape
    total = members * mem_n
    nobs = obs_x.shape[0]
    chips = mem_n // 2
    row = lax.axis_index("rows")
    mem = lax.axis_index("mem")
    core = lax.rem(mem, 2)
    chip = mem // 2
    partner = chip * 2 + 1 - core

    def dev(r, m):
        return {"rows": r, "mem": m}

    def remote(src, dst, ssem, rsem, r, m):
        return pltpu.make_async_remote_copy(
            src_ref=src, dst_ref=dst, send_sem=ssem, recv_sem=rsem,
            device_id=(r, m), device_id_type=MESH,
        )

    barrier = pltpu.get_barrier_semaphore()
    for d in range(1, mem_n):
        pl.semaphore_signal(barrier, inc=1, device_id=(row, lax.rem(mem + d, mem_n)), device_id_type=MESH)
    for d in range(1, rows_n):
        pl.semaphore_signal(barrier, inc=1, device_id=(lax.rem(row + d, rows_n), mem), device_id_type=MESH)
    pl.semaphore_wait(barrier, mem_n - 1 + rows_n - 1)

    has_low = row > 0
    has_high = row < rows_n - 1
    low = jnp.maximum(row - 1, 0)
    high = jnp.minimum(row + 1, rows_n - 1)

    def chalo_up():
        return remote(cour.at[:, rows - 2 + core], chalo.at[0, core], c_send.at[0], c_recv.at[0], high, mem)

    def chalo_down():
        return remote(cour.at[:, core], chalo.at[1, core], c_send.at[1], c_recv.at[1], low, mem)

    def chalo_pass(side):
        return remote(chalo.at[side, core], chalo.at[side, core], cf_send.at[side], cf_recv.at[side], row, partner)

    def halo_up(m):
        return remote(ens.at[m, pl.ds(rows - 3, 3)], hal.at[m, 0], h_send.at[0, m], h_recv.at[0, m], high, mem)

    def halo_down(m):
        return remote(ens.at[m, pl.ds(0, 3)], hal.at[m, 1], h_send.at[1, m], h_recv.at[1, m], low, mem)

    @pl.when(has_high)
    def _():
        chalo_up().start()

    @pl.when(has_low)
    def _():
        chalo_down().start()

    def send_halo(m):
        @pl.when(has_high)
        def _():
            halo_up(m).start()

        @pl.when(has_low)
        def _():
            halo_down(m).start()

    ahead = min(AHEAD, members)

    @pl.loop(0, ahead)
    def _(m):
        send_halo(m)

    level = lax.broadcasted_iota(jnp.int32, (levels, width), 0)
    cell = lax.broadcasted_iota(jnp.int32, (levels, width), 1)

    def set_coef(i, a0, a1, a2):
        coef[i, 0] = 1.0 - 6.0 * DIFFUSION - jnp.abs(a0) - jnp.abs(a1) - jnp.abs(a2)
        coef[i, 1] = DIFFUSION + jnp.maximum(a0, 0.0)
        coef[i, 2] = DIFFUSION - jnp.minimum(a0, 0.0)
        coef[i, 3] = jnp.where(cell > 0, DIFFUSION + jnp.maximum(a1, 0.0), 0.0)
        coef[i, 4] = jnp.where(cell < width - 1, DIFFUSION - jnp.minimum(a1, 0.0), 0.0)
        coef[i, 5] = jnp.where(level > 0, DIFFUSION + jnp.maximum(a2, 0.0), 0.0)
        coef[i, 6] = jnp.where(level < levels - 1, DIFFUSION - jnp.minimum(a2, 0.0), 0.0)

    @pl.loop(0, rows)
    def _(i):
        set_coef(i + 2, cour[0, i], cour[1, i], cour[2, i])

    st[...] = jnp.zeros_like(st)

    def edge(side, present, first):
        @pl.when(present)
        def _():
            (chalo_down if side else chalo_up)().wait_recv()
            chalo_pass(side).start()
            chalo_pass(side).wait_recv()

            @pl.loop(0, 2)
            def _(i):
                set_coef(first + i, chalo[side, i, 0], chalo[side, i, 1], chalo[side, i, 2])

        @pl.when(jnp.logical_not(present))
        def _():
            coef[pl.ds(first, 2)] = jnp.zeros((2, 7, levels, width), jnp.float32)

    edge(0, has_low, 0)
    edge(1, has_high, rows + 2)

    @pl.when(jnp.logical_not(has_low))
    def _():
        w0[pl.ds(0, 3)] = jnp.zeros((3, levels, width), jnp.float32)

    @pl.when(jnp.logical_not(has_high))
    def _():
        w0[pl.ds(rows + 3, 3)] = jnp.zeros((3, levels, width), jnp.float32)

    def update(src, i, c):
        mid = src[i + 1]
        return (
            coef[c, 0] * mid
            + coef[c, 1] * src[i]
            + coef[c, 2] * src[i + 2]
            + coef[c, 3] * pltpu.roll(mid, 1, 1)
            + coef[c, 4] * pltpu.roll(mid, width - 1, 1)
            + coef[c, 5] * pltpu.roll(mid, 1, 0)
            + coef[c, 6] * pltpu.roll(mid, levels - 1, 0)
        )

    def other(d):
        return lax.rem(chip + d, chips) * 2 + core

    def send_x(d, m):
        slot = fc.at[mem * members + m]
        return remote(slot, slot, x_send.at[d, m], f_recv.at[mem, m], row, other(d))

    def send_p(d, m):
        src = lax.rem(chip + d, chips) * 2 + core
        slot = fc.at[src * members + m]
        return remote(slot, slot, p_send.at[d, m], f_recv.at[src, m], row, partner)

    def arrived(src, m):
        slot = fc.at[src * members + m]
        return remote(slot, slot, p_send.at[0, 0], f_recv.at[src, m], row, partner)

    def forward(m):
        for d in range(1, chips):
            arrived(other(d), m).wait_recv()
            send_p(d, m).start()

    lane = lax.broadcasted_iota(jnp.int32, (levels, LANES), 1)
    lag = 2

    @pl.loop(0, members)
    def _(m):
        @pl.when(has_low)
        def _():
            halo_up(m).wait_recv()
            w0[pl.ds(0, 3)] = hal[m, 0]

        @pl.when(has_high)
        def _():
            halo_down(m).wait_recv()
            w0[pl.ds(rows + 3, 3)] = hal[m, 1]

        @pl.when(m + ahead < members)
        def _():
            send_halo(m + ahead)

        w0[pl.ds(3, rows)] = ens[m]

        @pl.loop(0, rows + 4, unroll=2)
        def _(i):
            w1[i] = update(w0, i, i)

        @pl.loop(0, rows + 2, unroll=2)
        def _(i):
            w2[i] = update(w1, i, i + 1)

        @pl.loop(0, rows, unroll=2)
        def _(i):
            value = update(w2, i, i + 2)
            w3[i] = value
            fc[mem * members + m, i] = value

        @pl.loop(0, nobs, unroll=4)
        def _(p):
            plane = w3[obs_x[p]]
            hit = cell == obs_y[p]
            picked = jnp.sum(jnp.where(hit, plane, 0.0), axis=1, keepdims=True)
            where = pl.ds(pl.multiple_of(p * levels, levels), levels)
            st[where] = jnp.where(lane == m, picked, st[where])

        for d in range(1, chips):
            send_x(d, m).start()
        send_p(0, m).start()

        @pl.when(m >= lag)
        def _():
            forward(m - lag)

    def dot(a, b):
        return jnp.dot(a, b, precision=HIGHEST, preferred_element_type=jnp.float32)

    def flat(ref):
        n = nobs * levels
        spread = lax.broadcasted_iota(jnp.int32, (levels, n), 1) % levels
        spread = jnp.where(spread == lax.broadcasted_iota(jnp.int32, (levels, n), 0), 1.0, 0.0)
        wide = dot(ref[...], spread.astype(jnp.float32))
        owner = lax.broadcasted_iota(jnp.int32, (nobs, n), 1) // levels
        own = owner == lax.broadcasted_iota(jnp.int32, (nobs, n), 0)
        return jnp.sum(jnp.where(own, wide, 0.0), axis=0, keepdims=True)

    mine = pl.ds(pl.multiple_of(mem * members, members), members)
    prof[mine] = st[...].T[:members]
    for d in range(1, mem_n):
        remote(prof.at[mine], prof.at[mine], q_send.at[d], q_recv.at[mem], row, lax.rem(mem + d, mem_n)).start()
    for d in range(1, mem_n):
        src = lax.rem(mem + d, mem_n)
        block = prof.at[pl.ds(pl.multiple_of(src * members, members), members)]
        remote(block, block, q_send.at[d], q_recv.at[src], row, src).wait_recv()

    values = prof[...]
    variance = flat(obs_var)
    center = jnp.mean(values, axis=0, keepdims=True)
    scaled = (values - center) / jnp.sqrt((total - 1.0) * variance)
    innovation = (flat(obs_value) - center) / jnp.sqrt(variance)
    pad = jnp.broadcast_to(innovation, (LANES - total, innovation.shape[1]))
    both = jnp.concatenate([scaled, pad], axis=0)
    grec[row] = lax.dot_general(
        scaled, both, (((1,), (1,)), ((), ())), precision=HIGHEST, preferred_element_type=jnp.float32
    )
    for d in range(1, rows_n):
        remote(grec.at[row], grec.at[row], g_send.at[d], g_recv.at[row], lax.rem(row + d, rows_n), mem).start()

    forward(members - 2)
    forward(members - 1)

    for d in range(1, rows_n):
        src = lax.rem(row + d, rows_n)
        remote(grec.at[src], grec.at[src], g_send.at[d], g_recv.at[src], src, mem).wait_recv()
    gsum = grec[0]
    for r in range(1, rows_n):
        gsum = gsum + grec[r]

    ri = lax.broadcasted_iota(jnp.int32, (total, total), 0)
    ci = lax.broadcasted_iota(jnp.int32, (total, total), 1)
    eye = jnp.where(ri == ci, 1.0, 0.0).astype(jnp.float32)
    system = eye + gsum[:, :total]
    frob = jnp.sqrt(jnp.sum(jnp.sum(system * system, axis=1, keepdims=True), axis=0, keepdims=True))
    y = system / frob
    z = eye
    for it in range(NS_ITERS):
        factor = 0.5 * (3.0 * eye - (y if it == 0 else dot(z, y)))
        if it < NS_ITERS - 1:
            y = dot(y, factor)
        z = factor if it == 0 else dot(factor, z)
    root = z / jnp.sqrt(frob)
    shift = dot(root, dot(root, gsum))[:, total:total + 1] / jnp.sqrt(jnp.float32(total - 1.0))
    mixed = shift + root
    weights = 1.0 / total + mixed - jnp.mean(mixed, axis=0, keepdims=True)
    wts[...] = weights.T
    tile = 8
    outs, ins = members * tile, total * tile

    def hot(shape, dim, size):
        big = lax.broadcasted_iota(jnp.int32, shape, dim) // size
        return jnp.where(big == lax.broadcasted_iota(jnp.int32, shape, 1 - dim), 1.0, 0.0).astype(jnp.float32)

    wide = dot(dot(hot((outs, members), 0, tile), wts[mine]), hot((total, ins), 1, tile))
    same = (
        lax.broadcasted_iota(jnp.int32, (outs, ins), 0) % tile
        == lax.broadcasted_iota(jnp.int32, (outs, ins), 1) % tile
    )
    wide = jnp.where(same, wide, 0.0)
    wide_high = wide.astype(jnp.bfloat16)
    wide_low = (wide - wide_high.astype(jnp.float32)).astype(jnp.bfloat16)

    for d in range(chips):
        src = lax.rem(chip + d, chips) * 2 + 1 - core

        @pl.loop(0, members)
        def _(m):
            arrived(src, m).wait_recv()

    def dot16(a, b):
        return jnp.dot(a, b, preferred_element_type=jnp.float32)

    @pl.loop(0, rows * (levels // tile), unroll=2)
    def _(n):
        i = n // (levels // tile)
        where = pl.ds(pl.multiple_of(lax.rem(n, levels // tile) * tile, tile), tile)
        f = fc[:, i, where].reshape(ins, width)
        f_high = f.astype(jnp.bfloat16)
        f_low = (f - f_high.astype(jnp.float32)).astype(jnp.bfloat16)
        value = dot16(wide_high, f_high) + (dot16(wide_high, f_low) + dot16(wide_low, f_high))
        out[:, i, where] = value.reshape(members, tile, width)

    @pl.when(has_high)
    def _():
        chalo_up().wait_send()
        chalo_pass(1).wait_send()

    @pl.when(has_low)
    def _():
        chalo_down().wait_send()
        chalo_pass(0).wait_send()

    @pl.loop(0, members)
    def _(m):
        @pl.when(has_high)
        def _():
            halo_up(m).wait_send()

        @pl.when(has_low)
        def _():
            halo_down(m).wait_send()

        for d in range(1, chips):
            send_x(d, m).wait_send()
        for d in range(chips):
            send_p(d, m).wait_send()

    for d in range(1, mem_n):
        remote(prof.at[mine], prof.at[mine], q_send.at[d], q_recv.at[mem], row, lax.rem(mem + d, mem_n)).wait_send()
    for d in range(1, rows_n):
        remote(grec.at[row], grec.at[row], g_send.at[d], g_recv.at[row], lax.rem(row + d, rows_n), mem).wait_send()


def per_device(rows_n, mem_n, ensemble, courant, obs_column, obs_value, obs_var):
    members, levels, rows, width = ensemble.shape
    nobs = obs_column.shape[0]
    chips = mem_n // 2
    local = obs_column - lax.axis_index("rows") * (rows * width)
    f32 = jnp.float32
    vmem = pl.BlockSpec(memory_space=pltpu.VMEM)
    smem = pl.BlockSpec(memory_space=pltpu.SMEM)
    dma = pltpu.SemaphoreType.DMA
    total = members * mem_n
    plane = (levels, width)
    result = pl.pallas_call(
        functools.partial(kernel, rows_n, mem_n),
        out_shape=jax.ShapeDtypeStruct((members, rows, levels, width), f32),
        in_specs=[vmem, vmem, smem, smem, vmem, vmem],
        out_specs=vmem,
        scratch_shapes=[
            pltpu.VMEM((2, 2, 3) + plane, f32),
            pltpu.VMEM((members, 2, 3) + plane, f32),
            pltpu.VMEM((rows + 4, 7) + plane, f32),
            pltpu.VMEM((rows + 6,) + plane, f32),
            pltpu.VMEM((rows + 4,) + plane, f32),
            pltpu.VMEM((rows + 2,) + plane, f32),
            pltpu.VMEM((rows,) + plane, f32),
            pltpu.VMEM((total, rows) + plane, f32),
            pltpu.VMEM((nobs * levels, LANES), f32),
            pltpu.VMEM((total, nobs * levels), f32),
            pltpu.VMEM((rows_n, total, LANES), f32),
            pltpu.VMEM((total, total), f32),
            dma((2,)), dma((2,)), dma((2,)), dma((2,)),
            dma((2, members)), dma((2, members)),
            dma((chips, members)), dma((chips, members)), dma((mem_n, members)),
            dma((mem_n,)), dma((mem_n,)),
            dma((rows_n,)), dma((rows_n,)),
        ],
        compiler_params=pltpu.CompilerParams(
            collective_id=0, has_side_effects=True, vmem_limit_bytes=60 * 1024 * 1024
        ),
    )(
        ensemble.transpose(0, 2, 1, 3),
        courant.transpose(0, 2, 1, 3),
        local // width,
        local % width,
        obs_value.T,
        obs_var.T,
    )
    return result.transpose(0, 2, 1, 3)


def solution(mesh):
    return jax.shard_map(
        functools.partial(per_device, mesh.shape["rows"], mesh.shape["mem"]),
        mesh=mesh,
        in_specs=(
            P("mem", None, "rows", None),
            P(None, None, "rows", None),
            P("rows"),
            P(None, "rows"),
            P(None, "rows"),
        ),
        out_specs=P("mem", None, "rows", None),
        check_vma=False,
    )
```
